256 devices in a mesh: seq: 256 (over x, y, z, core).
Axes of the slice: x: 4, y: 4, z: 8, core: 2. Of those that a mesh axis runs over, the one named last changes fastest.
Arguments:
- history: float32 [98304, 1024], P('seq'), may hold values from -6 to 6
- taps: float32 [98304, 1024], P('seq'), may hold values from -0.078125 to 0.078125
- self_taps: float32 [1024, 256], P('seq'), may hold values from -0.375 to 0.375
- fresh: float32 [1024, 256], P('seq'), may hold values from -6 to 6
- gate: float32 [1024, 256], P('seq'), may hold values from -6 to 6
Outputs:
- gated: float32 [1024, 256], P('seq')
The draws below stay inside these ranges and needn't reach their ends.
All inputs are finite; a program needn't handle non-finite values.
Results may differ from the reference program's by a relative error of at most 0.000053.
Values sent between devices are 32-bit elements; how exact they have to be, the bound alone decides.
No kernel may reach another device: no remote copies, remote signals or barrier semaphores. Data moves between devices by JAX's collectives and lax.ppermute only.
A program may use at most 64 MiB of HBM per device.

```python
import jax
import jax.numpy as jnp
from jax import lax

CHANNELS = 1024
NEW_TOKENS = 256
HISTORY = 98304


def raised(entries, key, source, target, shards_of, factor):
    owner, partner = [(jnp.arange(entries.shape[dim]) // (entries.shape[dim] // shards_of)).reshape([-1 if axis == dim else 1 for axis in range(entries.ndim)]) for dim in (source, target)]
    chosen = jax.random.permutation(key, shards_of)[partner]
    strong = (owner == chosen) | (owner == (partner + shards_of // 2) % shards_of)
    return jnp.where(strong, factor * entries, entries)


def steps_of(own_key, shape, shards, smallest, high):
    gain, own = 1.0, jax.random.fold_in(own_key, 6)
    for dim, shards_of in shards:
        heights = jnp.exp(jax.random.uniform(jax.random.fold_in(own, dim), (shards_of,), jnp.float32, smallest / len(shards), high / len(shards)))
        gain = gain * jnp.repeat(heights, shape[dim] // shards_of).reshape([-1 if axis == dim else 1 for axis in range(len(shape))])
    return gain


def gaussian(rng, shape, deviation, reach, split=(), dtype=jnp.bfloat16):
    level = steps_of(rng, shape, split, -0.22, 0.18) if split else 1.0
    entries = jax.random.normal(rng, shape, jnp.float32) * deviation * level
    return jnp.minimum(jnp.maximum(entries, -reach), reach).astype(dtype)


def heavy_noise(own_key, shape, spread, most, split, heavy, held_as=jnp.bfloat16):
    array = spread * jax.random.normal(own_key, shape, jnp.float32)
    if split:
        array = array * steps_of(own_key, shape, split, -0.22, 0.18)
    return jnp.clip(raised(array, jax.random.fold_in(own_key, 3), *heavy), -most, most).astype(held_as)


def setup_inputs(seed: int = 0) -> dict:
    arg_keys = jax.random.split(jax.random.key(seed), 6)
    return {
        "history": gaussian(arg_keys[0], (HISTORY, CHANNELS), 1.0, 6.0, ((0, 256),), jnp.float32),
        "taps": heavy_noise(arg_keys[1], (HISTORY, CHANNELS), HISTORY ** -0.5, 0.078125, ((0, 256),), (0, 1, 256, 6.0), jnp.float32),
        "self_taps": gaussian(arg_keys[2], (CHANNELS, NEW_TOKENS), NEW_TOKENS ** -0.5, 0.375, ((0, 256),), jnp.float32),
        "fresh": gaussian(arg_keys[3], (CHANNELS, NEW_TOKENS), 1.0, 6.0, ((0, 256),), jnp.float32),
        "gate": gaussian(arg_keys[4], (CHANNELS, NEW_TOKENS), 1.0, 6.0, ((0, 256),), jnp.float32),
    }


def correlate(pair):
    hist_block, taps_block = pair
    length = 2 * HISTORY
    hist_spec = jnp.fft.rfft(hist_block, n=length, axis=0)
    taps_spec = jnp.fft.rfft(taps_block, n=length, axis=0)
    return jnp.fft.irfft(jnp.conj(taps_spec) * hist_spec, n=length, axis=0)[:NEW_TOKENS]


def reference(history, taps, self_taps, fresh, gate):
    groups = CHANNELS // 32
    hist_blocks = history.reshape(HISTORY, groups, 32).transpose(1, 0, 2)
    taps_blocks = taps.reshape(HISTORY, groups, 32).transpose(1, 0, 2)
    lagged = lax.map(correlate, (hist_blocks, taps_blocks))
    hist_part = lagged.transpose(0, 2, 1).reshape(CHANNELS, NEW_TOKENS)
    doubled = 2 * NEW_TOKENS
    own_spec = jnp.fft.rfft(self_taps, n=doubled, axis=1) * jnp.fft.rfft(fresh, n=doubled, axis=1)
    own_part = jnp.fft.irfft(own_spec, n=doubled, axis=1)[:, :NEW_TOKENS]
    return gate * (hist_part + own_part)
```

```python
import functools
import math

import jax
import jax.numpy as jnp
import numpy as np
from jax import lax
from jax.experimental import pallas as pl
from jax.experimental.pallas import tpu as pltpu
from jax.sharding import Mesh
from jax.sharding import PartitionSpec as P

AXES = ("x", "y", "z", "c")
BLOCK = 128
LENGTH = 384
HALF = 200
TILE = 256


def split(values):
    high = values.astype(jnp.bfloat16)
    low = (values - high.astype(jnp.float32)).astype(jnp.bfloat16)
    return high, low


def stacked(values):
    high, low = split(values)
    return jnp.concatenate([high, low, high], axis=0)


def tables(new_len):
    def parts(array):
        high = array.astype(jnp.bfloat16)
        low = (array - high.astype(np.float64)).astype(jnp.bfloat16)
        return high, low

    freq = np.arange(HALF)
    used = freq <= LENGTH // 2
    angle = 2.0 * math.pi / LENGTH * (np.outer(freq, np.arange(BLOCK)) % LENGTH)
    forward = np.concatenate([np.cos(angle), np.sin(angle)]) * np.tile(used, 2)[:, None]
    high, low = parts(forward)
    forward = np.concatenate([high, high, low], axis=1)
    weight = used * np.where((freq == 0) | (freq == LENGTH // 2), 1.0, 2.0) / LENGTH
    angle = 2.0 * math.pi / LENGTH * (np.outer(np.arange(new_len), freq) % LENGTH)
    inverse = np.concatenate([np.cos(angle) * weight, np.sin(angle) * weight], axis=1)
    high, low = parts(inverse)
    inverse = np.concatenate([high, high, low], axis=1)
    turn = 2.0 * math.pi / 3.0 * (freq % 3)
    turn = np.stack([np.cos(turn), np.sin(turn)])[:, :, None]
    turn = np.broadcast_to(turn, (2, HALF, TILE)).astype(np.float32)
    return forward, inverse, turn


def dot(left, right):
    return jnp.dot(left, right, preferred_element_type=jnp.float32)


def local_kernel(
    hist_ref, taps_ref, forward_ref, turn_ref, self_ref, fresh_ref, spec_ref, near_ref, far_ref, own_ref
):
    forward = forward_ref[...]
    cos, sin = turn_ref[0], turn_ref[1]

    def spectrum(ref, block):
        both = dot(forward, stacked(ref[block * BLOCK : (block + 1) * BLOCK, :]))
        return both[:HALF], both[HALF:]

    a0, b0 = spectrum(taps_ref, 0)
    x0, y0 = spectrum(hist_ref, 0)
    real = x0 * a0 + y0 * b0
    imag = y0 * a0 - x0 * b0
    ca, sb, cb, sa = cos * a0, sin * b0, cos * b0, sin * a0
    back_a, back_b = ca + sb, cb - sa
    on_a, on_b = ca - sb, cb + sa
    x1, y1 = spectrum(hist_ref, 1)
    near_ref[:HALF, :] = cos * (x0 + x1) - sin * (y0 - y1)
    near_ref[HALF:, :] = cos * (y0 + y1) + sin * (x0 - x1)
    a1, b1 = spectrum(taps_ref, 1)
    a, b = a1 + back_a, b1 + back_b
    real += x1 * a + y1 * b
    imag += y1 * a - x1 * b
    ca, sb, cb, sa = cos * a1, sin * b1, cos * b1, sin * a1
    far_ref[:HALF, :] = ca - sb
    far_ref[HALF:, :] = cb + sa
    on_a, on_b = on_a + ca + sb, on_b + cb - sa
    a2, b2 = spectrum(taps_ref, 2)
    x2, y2 = spectrum(hist_ref, 2)
    a, b = a2 + on_a, b2 + on_b
    spec_ref[:HALF, :] = real + x2 * a + y2 * b
    spec_ref[HALF:, :] = imag + y2 * a - x2 * b

    @pl.when(pl.program_id(0) == 0)
    def _():
        count, length = fresh_ref.shape
        for channel in range(count):
            row = self_ref[channel : channel + 1, :]
            row = jnp.concatenate([row, jnp.zeros_like(row)], axis=1)
            row = jnp.broadcast_to(row, (length, 2 * length))
            shifted = pltpu.roll(row, 0, 1, stride=1, stride_axis=0)[:, :length]
            high, low = split(shifted)
            fresh_high, fresh_low = split(fresh_ref[channel : channel + 1, :])
            own_ref[channel : channel + 1, :] = (
                dot(fresh_high, high) + dot(fresh_high, low) + dot(fresh_low, high)
            )


def halo_kernel(
    core_ref, spec_ref, near_ref, far_ref, taps_ref, hist_ref, forward_ref, inverse_ref, keep_ref, send_ref
):
    forward = forward_ref[...]
    both = dot(forward, stacked(taps_ref[...]))
    a, b = both[:HALF], both[HALF:]
    near_x, near_y = near_ref[:HALF, :], near_ref[HALF:, :]
    real = spec_ref[:HALF, :] + near_x * a + near_y * b
    imag = spec_ref[HALF:, :] + near_y * a - near_x * b
    both = dot(forward, stacked(hist_ref[...]))
    x, y = both[:HALF], both[HALF:]
    far_a, far_b = far_ref[:HALF, :], far_ref[HALF:, :]
    real += x * far_a + y * far_b
    imag += y * far_a - x * far_b
    out = dot(inverse_ref[...], stacked(jnp.concatenate([real, imag], axis=0))).T
    channels, length = out.shape
    out = out.reshape(channels // 16, 2, 8, length)
    even, odd = out[:, 0], out[:, 1]
    row = lax.broadcasted_iota(jnp.int32, even.shape, 1)
    first = jnp.where(row < 4, even, pltpu.roll(odd, 4, 1)).reshape(channels // 2, length)
    second = jnp.where(row < 4, pltpu.roll(even, 4, 1), odd).reshape(channels // 2, length)

    @pl.when(core_ref[0] == 0)
    def _():
        keep_ref[...] = first
        send_ref[...] = second

    @pl.when(core_ref[0] != 0)
    def _():
        keep_ref[...] = second
        send_ref[...] = first


def body(history, taps, self_taps, fresh, gate):
    rows, channels = history.shape
    mine, new_len = fresh.shape
    forward, inverse, turn = tables(new_len)
    sizes = [lax.axis_size(axis) for axis in AXES]
    count = math.prod(sizes)
    onward = [(source, source + 1) for source in range(count - 1)]
    back = [(target, source) for source, target in onward]
    before = lax.ppermute(taps[rows - BLOCK :], AXES, onward)
    after = lax.ppermute(history[:BLOCK], AXES, back)

    steps = channels // TILE
    columns = lambda height: pl.BlockSpec((height, TILE), lambda i: (0, i))
    whole = lambda array: pl.BlockSpec(array.shape, lambda i: (0,) * array.ndim)
    wide = jax.ShapeDtypeStruct((2 * HALF, channels), jnp.float32)
    spec, near, far, own = pl.pallas_call(
        local_kernel,
        grid=(steps,),
        in_specs=[columns(rows), columns(rows), whole(forward), whole(turn), whole(self_taps), whole(fresh)],
        out_specs=[columns(2 * HALF)] * 3 + [whole(fresh)],
        out_shape=[wide] * 3 + [jax.ShapeDtypeStruct(fresh.shape, jnp.float32)],
        compiler_params=pltpu.CompilerParams(vmem_limit_bytes=32 * 2**20),
        cost_estimate=pl.CostEstimate(flops=4 * 10**9, bytes_accessed=8 * 10**6, transcendentals=0),
        name="local",
    )(history, taps, forward, turn, self_taps, fresh)
    core = lax.axis_index("c").reshape(1)
    half = jax.ShapeDtypeStruct((channels // 2, new_len), jnp.float32)
    keep, send = pl.pallas_call(
        halo_kernel,
        grid=(steps,),
        in_specs=[pl.BlockSpec(memory_space=pltpu.SMEM)]
        + [columns(2 * HALF)] * 3
        + [columns(BLOCK)] * 2
        + [whole(forward), whole(inverse)],
        out_specs=[pl.BlockSpec((TILE // 2, new_len), lambda i: (i, 0))] * 2,
        out_shape=[half] * 2,
        compiler_params=pltpu.CompilerParams(vmem_limit_bytes=32 * 2**20),
        cost_estimate=pl.CostEstimate(flops=2 * 10**9, bytes_accessed=8 * 10**6, transcendentals=0),
        name="halo",
    )(core, spec, near, far, before, after, forward, inverse)
    joined = keep + lax.ppermute(send, "c", [(0, 1), (1, 0)])
    plane = sizes[0] * sizes[1]
    blocks = joined.reshape(plane, -1, new_len)
    blocks = lax.all_to_all(blocks, ("x", "y"), split_axis=0, concat_axis=0, tiled=True)
    column = blocks.sum(axis=0).reshape(sizes[2], mine, new_len)
    column = lax.all_to_all(column, "z", split_axis=0, concat_axis=0, tiled=True)
    return gate * (column.sum(axis=0) + own)


def solution(mesh):
    finer = Mesh(mesh.devices.reshape(4, 4, 8, 2), AXES)
    specs = P(AXES, None)
    return jax.shard_map(body, mesh=finer, in_specs=(specs,) * 5, out_specs=specs, check_vma=False)
```
